256 devices in a mesh: batch: 64 (over z, y, core), group: 4 (over x).
Axes of the slice: x: 4, y: 4, z: 8, core: 2. Of those that a mesh axis runs over, the one named last changes fastest.
Arguments:
- samples_in: float32 [16384, 8192], P('batch', 'group'), may hold values from -8 to 8, as said below
- second_samples_in: float32 [16384, 8192], P('batch', 'group'), may hold values from -8 to 8, as said below
Outputs:
- standard: float32 [16384, 8192], P(None, ('group', 'batch'))
- second_standard: float32 [16384, 8192], P(None, ('group', 'batch'))
The draws below stay inside these ranges and needn't reach their ends.
Inputs may be any that keep to these rules, and one draw needn't show every extreme that they name: samples_in holds numbers from -8 to 8. second_samples_in holds numbers from -8 to 8.
All inputs are finite; a program needn't handle non-finite values.
Results may differ from the reference program's by a relative error of at most 0.0003.
Values sent between devices are 32-bit elements.
A program may use at most 64 MiB of HBM per device.

```python
import jax
import jax.numpy as jnp

ROW_DEV = 256
ROWS = 16384
COLS = 8192
N_BATCH = 64


def column_values(key, tag):
    keys = jax.random.split(jax.random.fold_in(key, tag), 4)
    level = jax.random.normal(keys[0], (1, 1, COLS), jnp.float32) * 1.0
    spread = jnp.exp(jax.random.uniform(keys[1], (1, 1, COLS), jnp.float32, -0.7, 0.7))
    drift = jax.random.normal(keys[2], (N_BATCH, 1, COLS), jnp.float32) * 1.0
    noise = jax.random.normal(keys[3], (N_BATCH, ROW_DEV, COLS), jnp.float32) * 0.6
    return level + spread * (drift + noise)


def draw_samples_in(key, part):
    values = column_values(key, 1)
    return jnp.clip(values, -8.0, 8.0).reshape(ROWS, COLS)


def draw_second_samples_in(key, part):
    values = column_values(key, 2)
    return jnp.clip(values, -8.0, 8.0).reshape(ROWS, COLS)


def setup_inputs(seed: int = 0) -> dict:
    key_list = jax.random.split(jax.random.key(seed), 3)
    return {
        "samples_in": draw_samples_in(jax.random.fold_in(key_list[2], 71), 0),
        "second_samples_in": draw_second_samples_in(jax.random.fold_in(key_list[2], 71), 0),
    }


def reference(samples_in, second_samples_in):
    wide_standard = samples_in.astype(jnp.float32)
    low_standard = jnp.mean(jnp.minimum(wide_standard, 1.0), axis=0)
    high_standard = jnp.mean(jnp.maximum(wide_standard, 1.0), axis=0)
    standard = ((wide_standard - low_standard) / (high_standard - low_standard + 0.1))
    wide_second_standard = second_samples_in.astype(jnp.float32)
    low_second_standard = jnp.mean(jnp.minimum(wide_second_standard, 1.0), axis=0)
    high_second_standard = jnp.mean(jnp.maximum(wide_second_standard, 1.0), axis=0)
    second_standard = ((wide_second_standard - low_second_standard) / (high_second_standard - low_second_standard + 0.1))
    return standard, second_standard
```

```python
import jax
import jax.numpy as jnp
from jax import lax
from jax.experimental import pallas as pl
from jax.experimental.pallas import tpu as pltpu
from jax.sharding import PartitionSpec as P

MESH = pl.DeviceIdType.MESH
N = 64
ROWS, WIDE, NARROW = 256, 2048, 32
STEPS = (1, 7, 2, 6, 3, 5, 4, 0)


def device(me, dz, across):
    z, y, c = me // 8, (me // 2) % 4, me % 2
    return ((z + dz) % 8) * 8 + ((y + across % 4) % 4) * 2 + (c + across // 4) % 2


def kernel(a_ref, b_ref, first_out, second_out, held, turned, landed, in_sem, send_sem, recv_sem):
    me = lax.axis_index("batch")
    z = me // 8

    def load(which, step):
        columns = pl.ds(pl.multiple_of(((z + STEPS[step]) % 8) * ROWS, ROWS), ROWS)
        source = (a_ref, b_ref)[which]
        return pltpu.make_async_copy(
            source.at[:, columns], held.at[which, :, columns], in_sem.at[which, step]
        )

    for step in range(8):
        for which in range(2):
            load(which, step).start()

    barrier = pltpu.get_barrier_semaphore()

    def greet(i, carry):
        pl.semaphore_signal(
            barrier, inc=1, device_id={"batch": (me + i) % N}, device_id_type=MESH
        )
        return carry

    lax.fori_loop(1, N, greet, 0)

    def turn(step):
        zt = (z + STEPS[step]) % 8
        columns = pl.ds(pl.multiple_of(zt * ROWS, ROWS), ROWS)
        for which in range(2):
            load(which, step).wait()
            block = held[which, :, columns].T
            turned[pl.ds(zt * 8, 8), which * NARROW : (which + 1) * NARROW, :] = block.reshape(
                8, NARROW, ROWS
            )

    def send(round_, step):
        to = device(me, STEPS[step], (step + round_) % 8)
        pltpu.make_async_remote_copy(
            src_ref=turned.at[to],
            dst_ref=landed.at[me],
            send_sem=send_sem,
            recv_sem=recv_sem.at[round_],
            device_id={"batch": to},
            device_id_type=MESH,
        ).start()

    turn(0)
    pl.semaphore_wait(barrier, N - 1)
    for step in range(1, 8):
        turn(step)
        send(0, step - 1)
    send(0, 7)

    def send_round(round_, carry):
        for step in range(7):
            send(round_, step)

        @pl.when(round_ != 1)
        def _():
            send(round_, 7)

        return carry

    lax.fori_loop(1, 8, send_round, 0)

    def add(block, sums):
        low, high = sums
        left, right = block[:, :128], block[:, 128:]
        low = low + (jnp.minimum(left, 1.0) + jnp.minimum(right, 1.0))
        high = high + (jnp.maximum(left, 1.0) + jnp.maximum(right, 1.0))
        return low, high

    landed[me] = turned[me]
    sums = (jnp.zeros((2 * NARROW, 128), jnp.float32),) * 2
    sums = add(turned[me], sums)

    def came(round_, step):
        over = (step + round_) % 8
        return device(me, 8 - STEPS[step], (4 - over % 4) % 4 + 4 * (over // 4))

    def take(round_, sums, steps):
        for step in steps:
            sums = add(landed[came(round_, step)], sums)
        return sums

    for round_ in range(8):
        count = 7 if round_ == 1 else 8
        pltpu.make_async_copy(
            landed.at[pl.ds(0, count)], landed.at[pl.ds(0, count)], recv_sem.at[round_]
        ).wait()
        sums = take(round_, sums, range(count))

    low = jnp.sum(sums[0], axis=1, keepdims=True) * (1.0 / (N * ROWS))
    high = jnp.sum(sums[1], axis=1, keepdims=True) * (1.0 / (N * ROWS))
    scale = 1.0 / (high - low + 0.1)

    def finish(i, carry):
        block = (landed[i] - low) * scale
        rows = pl.ds(pl.multiple_of(i * ROWS, ROWS), ROWS)
        first_out[:, rows] = block[:NARROW]
        second_out[:, rows] = block[NARROW:]
        return carry

    lax.fori_loop(0, N, finish, 0, unroll=4)
    pltpu.make_async_copy(
        landed.at[pl.ds(0, N - 1)], landed.at[pl.ds(0, N - 1)], send_sem
    ).wait()


def shards(samples_in, second_samples_in):
    out = pltpu.VMEM((NARROW, N * ROWS), jnp.float32)
    first, second = pl.pallas_call(
        kernel,
        out_shape=(out, out),
        in_specs=[pl.BlockSpec(memory_space=pltpu.HBM)] * 2,
        out_specs=(pl.BlockSpec(memory_space=pltpu.VMEM),) * 2,
        scratch_shapes=[
            pltpu.VMEM((2, ROWS, WIDE), jnp.float32),
            pltpu.VMEM((N, 2 * NARROW, ROWS), jnp.float32),
            pltpu.VMEM((N, 2 * NARROW, ROWS), jnp.float32),
            pltpu.SemaphoreType.DMA((2, 8)),
            pltpu.SemaphoreType.DMA,
            pltpu.SemaphoreType.DMA((8,)),
        ],
        compiler_params=pltpu.CompilerParams(
            collective_id=0, has_side_effects=True, vmem_limit_bytes=59 * 2**20
        ),
    )(samples_in, second_samples_in)
    return first.T, second.T


def solution(mesh):
    placed = (P("batch", "group"), P("batch", "group"))
    return jax.shard_map(
        shards,
        mesh=mesh,
        in_specs=placed,
        out_specs=(P(None, ("group", "batch")), P(None, ("group", "batch"))),
        check_vma=False,
    )
```

```python
import jax
import jax.numpy as jnp
from jax import lax
from jax.experimental import pallas as pl
from jax.experimental.pallas import tpu as pltpu
from jax.sharding import PartitionSpec as P

MESH = pl.DeviceIdType.MESH
N = 64
ROWS, WIDE, NARROW = 256, 2048, 32
STEPS = (1, 7, 2, 6, 3, 5, 4, 0)
PAIR = 4 * NARROW


def kernel(
    a_ref, b_ref, landed, stats, held, turned, in_sem, send_sem, recv_sem, below, above, left, right
):
    me = lax.axis_index("batch")
    z, y, c = me // 8, (me // 2) % 4, me % 2

    def device(dz, dy, dc):
        return ((z + dz) % 8) * 8 + ((y + dy) % 4) * 2 + (c + dc) % 2

    def tell(sem, *offset):
        pl.semaphore_signal(
            sem, inc=1, device_id={"batch": device(*offset)}, device_id_type=MESH
        )

    barrier = pltpu.get_barrier_semaphore()
    neighbours = (
        (1, 0, 0), (1, 0, 1), (7, 0, 0), (7, 0, 1), (0, 0, 1), (0, 1, 0), (0, 3, 0)
    )
    for offset in neighbours:
        tell(barrier, *offset)

    def first_device(step, other):
        return ((z + STEPS[step]) % 8) * 8 + ((y // 2 + other) % 2) * 4

    def load(which, step, other):
        columns = pl.ds(pl.multiple_of(first_device(step, other) * NARROW, PAIR), PAIR)
        source = (a_ref, b_ref)[which]
        return pltpu.make_async_copy(
            source.at[:, columns], held.at[which, :, columns], in_sem.at[which, other, step]
        )

    for other in range(2):
        for step in range(8):
            for which in range(2):
                load(which, step, other).start()

    def turn(step, other):
        first = first_device(step, other)
        columns = pl.ds(pl.multiple_of(first * NARROW, PAIR), PAIR)
        for which in range(2):
            load(which, step, other).wait()
            block = held[which, :, columns].T
            turned[pl.ds(first, 4), which * NARROW : (which + 1) * NARROW, :] = block.reshape(
                4, NARROW, ROWS
            )

    def send(dz, dy, dc, group):
        to = device(dz, dy, dc)
        pltpu.make_async_remote_copy(
            src_ref=turned.at[to],
            dst_ref=landed.at[me],
            send_sem=send_sem,
            recv_sem=recv_sem.at[group],
            device_id={"batch": to},
            device_id_type=MESH,
        ).start()

    def send_column(step):
        send(STEPS[step], 0, 0, 0)
        send(STEPS[step], 0, 1, 0)

    turn(0, 0)
    turn(1, 0)
    pl.semaphore_wait(barrier, len(neighbours))
    tell(below, 1, 0, 0)
    tell(above, 7, 0, 0)
    send_column(0)
    turn(2, 0)
    send_column(1)
    pl.semaphore_wait(below, 1)
    tell(below, 1, 0, 0)
    pl.semaphore_wait(above, 1)
    tell(above, 7, 0, 0)
    turn(3, 0)
    send_column(2)
    turn(4, 0)
    send_column(3)
    pl.semaphore_wait(below, 1)
    tell(below, 1, 0, 0)
    pl.semaphore_wait(above, 1)
    turn(5, 0)
    send_column(4)
    turn(6, 0)
    send_column(5)
    pl.semaphore_wait(below, 1)
    tell(left, 0, 1, 0)
    tell(right, 0, 3, 0)
    turn(7, 0)
    send_column(6)
    turn(0, 1)
    send(0, 0, 1, 0)
    pl.semaphore_wait(left, 1)
    tell(left, 0, 1, 0)
    pl.semaphore_wait(right, 1)
    for step in range(1, 8):
        turn(step, 1)
    pl.semaphore_wait(left, 1)

    def over(round_, step):
        o = (step + round_) % 6
        return 1 + o % 3, o // 3

    def send_round(round_, carry):
        for step in range(8):
            dy, dc = over(round_, step)
            send(STEPS[step], dy, dc, 1 + round_)
        return carry

    lax.fori_loop(0, 6, send_round, 0)

    def add(block, sums):
        low, high = sums
        left, right = block[:, :128], block[:, 128:]
        low = low + (jnp.minimum(left, 1.0) + jnp.minimum(right, 1.0))
        high = high + (jnp.maximum(left, 1.0) + jnp.maximum(right, 1.0))
        return low, high

    def take(sums, dz, dy, dc):
        return add(landed[device(8 - dz, 4 - dy, dc)], sums)

    def wait(count, sem):
        pltpu.make_async_copy(landed.at[pl.ds(0, count)], landed.at[pl.ds(0, count)], sem).wait()

    landed[me] = turned[me]
    sums = (jnp.zeros((2 * NARROW, 128), jnp.float32),) * 2
    sums = add(turned[me], sums)
    wait(15, recv_sem.at[0])
    for dz in STEPS[:7]:
        for dc in range(2):
            sums = take(sums, dz, 0, dc)
    sums = take(sums, 0, 0, 1)

    def take_round(round_, sums):
        wait(8, recv_sem.at[1 + round_])
        for step in range(8):
            sums = take(sums, STEPS[step], *over(round_, step))
        return sums

    sums = lax.fori_loop(0, 6, take_round, sums)

    low = jnp.sum(sums[0], axis=1, keepdims=True) * (1.0 / (N * ROWS))
    high = jnp.sum(sums[1], axis=1, keepdims=True) * (1.0 / (N * ROWS))
    stats[0] = jnp.broadcast_to(low, stats.shape[1:])
    stats[1] = jnp.broadcast_to(1.0 / (high - low + 0.1), stats.shape[1:])
    wait(N - 1, send_sem)


def write(landed, stats, first_out, second_out, ready, sem):
    pieces = sem.shape[1]
    each = N // pieces

    def put(which, piece):
        out = (first_out, second_out)[which]
        rows = pl.ds(pl.multiple_of(piece * each * ROWS, each * ROWS), each * ROWS)
        return pltpu.make_async_copy(ready.at[which, :, rows], out.at[:, rows], sem.at[which, piece])

    low, factor = stats[0, :, :1], stats[1, :, :1]

    def finish(piece, carry):
        for i in range(each):
            block = (landed[piece * each + i] - low) * factor
            rows = pl.ds(pl.multiple_of((piece * each + i) * ROWS, ROWS), ROWS)
            ready[0, :, rows] = block[:NARROW]
            ready[1, :, rows] = block[NARROW:]
        put(0, piece).start()
        put(1, piece).start()
        return carry

    lax.fori_loop(0, pieces, finish, 0)

    def drain(piece, carry):
        put(0, piece).wait()
        put(1, piece).wait()
        return carry

    lax.fori_loop(0, pieces, drain, 0)


def shards(samples_in, second_samples_in):
    whole = pltpu.VMEM((N, 2 * NARROW, ROWS), jnp.float32)
    columns = pltpu.VMEM((2, 2 * NARROW, 128), jnp.float32)
    vmem, hbm = pl.BlockSpec(memory_space=pltpu.VMEM), pl.BlockSpec(memory_space=pltpu.HBM)
    landed, stats = pl.pallas_call(
        kernel,
        out_shape=(whole, columns),
        in_specs=[hbm] * 2,
        out_specs=(vmem,) * 2,
        scratch_shapes=[
            pltpu.VMEM((2, ROWS, WIDE), jnp.float32),
            whole,
            pltpu.SemaphoreType.DMA((2, 2, 8)),
            pltpu.SemaphoreType.DMA,
            pltpu.SemaphoreType.DMA((7,)),
            pltpu.SemaphoreType.REGULAR,
            pltpu.SemaphoreType.REGULAR,
            pltpu.SemaphoreType.REGULAR,
            pltpu.SemaphoreType.REGULAR,
        ],
        compiler_params=pltpu.CompilerParams(
            collective_id=0, has_side_effects=True, vmem_limit_bytes=58 * 2**20
        ),
    )(samples_in, second_samples_in)
    out = jax.ShapeDtypeStruct((NARROW, N * ROWS), jnp.float32)
    first, second = pl.pallas_call(
        write,
        out_shape=(out, out),
        in_specs=[vmem] * 2,
        out_specs=(hbm,) * 2,
        scratch_shapes=[
            pltpu.VMEM((2, NARROW, N * ROWS), jnp.float32),
            pltpu.SemaphoreType.DMA((2, 8)),
        ],
        compiler_params=pltpu.CompilerParams(vmem_limit_bytes=16 * 2**20),
    )(landed, stats)
    return first.T, second.T


def solution(mesh):
    placed = (P("batch", "group"), P("batch", "group"))
    return jax.shard_map(
        shards,
        mesh=mesh,
        in_specs=placed,
        out_specs=(P(None, ("group", "batch")), P(None, ("group", "batch"))),
        check_vma=False,
    )
```

```python
import jax
import jax.numpy as jnp
from jax import lax
from jax.experimental import pallas as pl
from jax.experimental.pallas import tpu as pltpu
from jax.sharding import PartitionSpec as P

MESH = pl.DeviceIdType.MESH
N = 64
ROWS, WIDE, NARROW = 256, 2048, 32
STEPS = (1, 7, 2, 6, 3, 5, 4, 0)
PAIR = 4 * NARROW


def kernel(
    a_ref, b_ref, landed, stats, held, turned, in_sem, send_sem, recv_sem, below, above, left, right
):
    me = lax.axis_index("batch")
    z, y, c = me // 8, (me // 2) % 4, me % 2

    def device(dz, dy, dc):
        return ((z + dz) % 8) * 8 + ((y + dy) % 4) * 2 + (c + dc) % 2

    def tell(sem, *offset):
        pl.semaphore_signal(
            sem, inc=1, device_id={"batch": device(*offset)}, device_id_type=MESH
        )

    barrier = pltpu.get_barrier_semaphore()
    neighbours = (
        (1, 0, 0), (1, 0, 1), (7, 0, 0), (7, 0, 1), (0, 0, 1), (0, 1, 0), (0, 3, 0)
    )
    for offset in neighbours:
        tell(barrier, *offset)

    def first_device(step, other):
        return ((z + STEPS[step]) % 8) * 8 + ((y // 2 + other) % 2) * 4

    def load(which, step, other):
        columns = pl.ds(pl.multiple_of(first_device(step, other) * NARROW, PAIR), PAIR)
        source = (a_ref, b_ref)[which]
        return pltpu.make_async_copy(
            source.at[:, columns], held.at[which, :, columns], in_sem.at[which, other, step]
        )

    for other in range(2):
        for step in range(8):
            for which in range(2):
                load(which, step, other).start()

    def turn(step, other):
        first = first_device(step, other)
        columns = pl.ds(pl.multiple_of(first * NARROW, PAIR), PAIR)
        for which in range(2):
            load(which, step, other).wait()
            block = held[which, :, columns].T
            turned[pl.ds(first, 4), which * NARROW : (which + 1) * NARROW, :] = block.reshape(
                4, NARROW, ROWS
            )

    def send(dz, dy, dc, group):
        to = device(dz, dy, dc)
        pltpu.make_async_remote_copy(
            src_ref=turned.at[to],
            dst_ref=landed.at[me],
            send_sem=send_sem,
            recv_sem=recv_sem.at[group],
            device_id={"batch": to},
            device_id_type=MESH,
        ).start()

    def send_column(step):
        send(STEPS[step], 0, 0, 0)
        send(STEPS[step], 0, 1, 0)

    turn(0, 0)
    turn(1, 0)
    pl.semaphore_wait(barrier, len(neighbours))
    tell(below, 1, 0, 0)
    tell(above, 7, 0, 0)
    send_column(0)
    turn(2, 0)
    send_column(1)
    pl.semaphore_wait(below, 1)
    tell(below, 1, 0, 0)
    pl.semaphore_wait(above, 1)
    tell(above, 7, 0, 0)
    turn(3, 0)
    send_column(2)
    turn(4, 0)
    send_column(3)
    pl.semaphore_wait(below, 1)
    tell(below, 1, 0, 0)
    pl.semaphore_wait(above, 1)
    turn(5, 0)
    send_column(4)
    turn(6, 0)
    send_column(5)
    pl.semaphore_wait(below, 1)
    tell(left, 0, 1, 0)
    tell(right, 0, 3, 0)
    turn(7, 0)
    send_column(6)
    turn(0, 1)
    send(0, 0, 1, 0)
    pl.semaphore_wait(left, 1)
    tell(left, 0, 1, 0)
    pl.semaphore_wait(right, 1)
    for step in range(1, 8):
        turn(step, 1)
    pl.semaphore_wait(left, 1)

    def over(round_, dz):
        m = (dz + 7) % 8
        o = (2 * m + (m // 4) * (13 - 4 * m) + 6 + round_) % 6
        return 1 + o // 2, o % 2

    def send_step(round_, dz):
        dy, dc = over(round_, dz)
        send(dz, dy, dc, 1 + round_)

    def to_half(q, half, k):
        send_step(q, (half * 4 + (z + k) % 4 + 8 - z) % 8)

    for q in range(4):
        for dz in STEPS:
            send_step(q, dz)
    for q in (4, 5):
        for half in range(2):
            for k in range(4):
                to_half(q, half, k)

    def add(block, sums):
        low, high = sums
        left, right = block[:, :128], block[:, 128:]
        low = low + (jnp.minimum(left, 1.0) + jnp.minimum(right, 1.0))
        high = high + (jnp.maximum(left, 1.0) + jnp.maximum(right, 1.0))
        return low, high

    def take(sums, dz, dy, dc):
        return add(landed[device(8 - dz, 4 - dy, dc)], sums)

    def wait(count, sem):
        pltpu.make_async_copy(landed.at[pl.ds(0, count)], landed.at[pl.ds(0, count)], sem).wait()

    landed[me] = turned[me]
    sums = (jnp.zeros((2 * NARROW, 128), jnp.float32),) * 2
    sums = add(turned[me], sums)
    wait(15, recv_sem.at[0])
    for dz in STEPS[:7]:
        for dc in range(2):
            sums = take(sums, dz, 0, dc)
    sums = take(sums, 0, 0, 1)

    def take_round(round_, sums):
        wait(8, recv_sem.at[1 + round_])
        for step in range(8):
            sums = take(sums, STEPS[step], *over(round_, STEPS[step]))
        return sums

    sums = lax.fori_loop(0, 6, take_round, sums)

    low = jnp.sum(sums[0], axis=1, keepdims=True) * (1.0 / (N * ROWS))
    high = jnp.sum(sums[1], axis=1, keepdims=True) * (1.0 / (N * ROWS))
    stats[0] = jnp.broadcast_to(low, stats.shape[1:])
    stats[1] = jnp.broadcast_to(1.0 / (high - low + 0.1), stats.shape[1:])
    wait(N - 1, send_sem)


def write(landed, stats, first_out, second_out, ready, sem):
    pieces = sem.shape[1]
    each = N // pieces

    def put(which, piece):
        out = (first_out, second_out)[which]
        rows = pl.ds(pl.multiple_of(piece * each * ROWS, each * ROWS), each * ROWS)
        return pltpu.make_async_copy(ready.at[which, :, rows], out.at[:, rows], sem.at[which, piece])

    low, factor = stats[0, :, :1], stats[1, :, :1]

    def finish(piece, carry):
        for i in range(each):
            block = (landed[piece * each + i] - low) * factor
            rows = pl.ds(pl.multiple_of((piece * each + i) * ROWS, ROWS), ROWS)
            ready[0, :, rows] = block[:NARROW]
            ready[1, :, rows] = block[NARROW:]
        put(0, piece).start()
        put(1, piece).start()
        return carry

    lax.fori_loop(0, pieces, finish, 0)

    def drain(piece, carry):
        put(0, piece).wait()
        put(1, piece).wait()
        return carry

    lax.fori_loop(0, pieces, drain, 0)


def shards(samples_in, second_samples_in):
    whole = pltpu.VMEM((N, 2 * NARROW, ROWS), jnp.float32)
    columns = pltpu.VMEM((2, 2 * NARROW, 128), jnp.float32)
    vmem, hbm = pl.BlockSpec(memory_space=pltpu.VMEM), pl.BlockSpec(memory_space=pltpu.HBM)
    landed, stats = pl.pallas_call(
        kernel,
        out_shape=(whole, columns),
        in_specs=[hbm] * 2,
        out_specs=(vmem,) * 2,
        scratch_shapes=[
            pltpu.VMEM((2, ROWS, WIDE), jnp.float32),
            whole,
            pltpu.SemaphoreType.DMA((2, 2, 8)),
            pltpu.SemaphoreType.DMA,
            pltpu.SemaphoreType.DMA((7,)),
            pltpu.SemaphoreType.REGULAR,
            pltpu.SemaphoreType.REGULAR,
            pltpu.SemaphoreType.REGULAR,
            pltpu.SemaphoreType.REGULAR,
        ],
        compiler_params=pltpu.CompilerParams(
            collective_id=0, has_side_effects=True, vmem_limit_bytes=58 * 2**20
        ),
    )(samples_in, second_samples_in)
    out = jax.ShapeDtypeStruct((NARROW, N * ROWS), jnp.float32)
    first, second = pl.pallas_call(
        write,
        out_shape=(out, out),
        in_specs=[vmem] * 2,
        out_specs=(hbm,) * 2,
        scratch_shapes=[
            pltpu.VMEM((2, NARROW, N * ROWS), jnp.float32),
            pltpu.SemaphoreType.DMA((2, 8)),
        ],
        compiler_params=pltpu.CompilerParams(vmem_limit_bytes=16 * 2**20),
    )(landed, stats)
    return first.T, second.T


def solution(mesh):
    placed = (P("batch", "group"), P("batch", "group"))
    return jax.shard_map(
        shards,
        mesh=mesh,
        in_specs=placed,
        out_specs=(P(None, ("group", "batch")), P(None, ("group", "batch"))),
        check_vma=False,
    )
```

```python
import jax
import jax.numpy as jnp
from jax import lax
from jax.experimental import pallas as pl
from jax.experimental.pallas import tpu as pltpu
from jax.sharding import PartitionSpec as P

MESH = pl.DeviceIdType.MESH
N = 64
ROWS, WIDE, NARROW = 256, 2048, 32
STEPS = (1, 7, 2, 6, 3, 5, 4, 0)
PAIR = 4 * NARROW


def kernel(
    a_ref, b_ref, landed, stats, held, turned, in_sem, send_sem, recv_sem, below, above, left, right
):
    me = lax.axis_index("batch")
    z, y, c = me // 8, (me // 2) % 4, me % 2

    def device(dz, dy, dc):
        return ((z + dz) % 8) * 8 + ((y + dy) % 4) * 2 + (c + dc) % 2

    def tell(sem, *offset):
        pl.semaphore_signal(
            sem, inc=1, device_id={"batch": device(*offset)}, device_id_type=MESH
        )

    barrier = pltpu.get_barrier_semaphore()
    neighbours = (
        (1, 0, 0), (1, 0, 1), (7, 0, 0), (7, 0, 1), (0, 0, 1), (0, 1, 0), (0, 3, 0)
    )
    for offset in neighbours:
        tell(barrier, *offset)

    sign = z // 2 % 2 * 2 - 1

    def turned_at(step):
        return (8 + sign * STEPS[step]) % 8

    def first_device(step, other):
        return ((z + turned_at(step)) % 8) * 8 + ((y // 2 + other) % 2) * 4

    def load(which, step, other):
        columns = pl.ds(pl.multiple_of(first_device(step, other) * NARROW, PAIR), PAIR)
        source = (a_ref, b_ref)[which]
        return pltpu.make_async_copy(
            source.at[:, columns], held.at[which, :, columns], in_sem.at[which, other, step]
        )

    for other in range(2):
        for step in range(8):
            for which in range(2):
                load(which, step, other).start()

    def turn(step, other):
        first = first_device(step, other)
        columns = pl.ds(pl.multiple_of(first * NARROW, PAIR), PAIR)
        for which in range(2):
            load(which, step, other).wait()
            block = held[which, :, columns].T
            turned[pl.ds(first, 4), which * NARROW : (which + 1) * NARROW, :] = block.reshape(
                4, NARROW, ROWS
            )

    def send(dz, dy, dc, group):
        to = device(dz, dy, dc)
        pltpu.make_async_remote_copy(
            src_ref=turned.at[to],
            dst_ref=landed.at[me],
            send_sem=send_sem,
            recv_sem=recv_sem.at[group],
            device_id={"batch": to},
            device_id_type=MESH,
        ).start()

    def send_column(step):
        send(turned_at(step), 0, 0, 0)
        send(turned_at(step), 0, 1, 0)

    turn(0, 0)
    pl.semaphore_wait(barrier, len(neighbours))
    tell(below, 1, 0, 0)
    tell(above, 7, 0, 0)
    send_column(0)
    turn(1, 0)
    send_column(1)
    turn(2, 0)
    pl.semaphore_wait(below, 1)
    tell(below, 1, 0, 0)
    pl.semaphore_wait(above, 1)
    tell(above, 7, 0, 0)
    send_column(2)
    turn(3, 0)
    send_column(3)
    turn(4, 0)
    pl.semaphore_wait(below, 1)
    tell(below, 1, 0, 0)
    pl.semaphore_wait(above, 1)
    send_column(4)
    turn(5, 0)
    send_column(5)
    turn(6, 0)
    pl.semaphore_wait(below, 1)
    tell(left, 0, 1, 0)
    tell(right, 0, 3, 0)
    turn(7, 0)
    send_column(6)
    turn(0, 1)
    send(0, 0, 1, 0)
    pl.semaphore_wait(left, 1)
    tell(left, 0, 1, 0)
    pl.semaphore_wait(right, 1)
    for step in range(1, 8):
        turn(step, 1)
    pl.semaphore_wait(left, 1)

    def over(round_, dz):
        m = (dz + 7) % 8
        o = (2 * m + (m // 4) * (13 - 4 * m) + 6 + round_) % 6
        return 1 + o // 2, o % 2

    def send_step(round_, dz):
        dy, dc = over(round_, dz)
        send(dz, dy, dc, 1 + round_)

    def to_half(q, half, k):
        send_step(q, (half * 4 + (z + k) % 4 + 8 - z) % 8)

    for q in range(4):
        for step in range(8):
            send_step(q, turned_at(step))
    for q in (4, 5):
        for half in range(2):
            for k in range(4):
                to_half(q, half, k)

    def add(block, sums):
        low, high = sums
        left, right = block[:, :128], block[:, 128:]
        low = low + (jnp.minimum(left, 1.0) + jnp.minimum(right, 1.0))
        high = high + (jnp.maximum(left, 1.0) + jnp.maximum(right, 1.0))
        return low, high

    def take(sums, dz, dy, dc):
        return add(landed[device(8 - dz, 4 - dy, dc)], sums)

    def wait(count, sem):
        pltpu.make_async_copy(landed.at[pl.ds(0, count)], landed.at[pl.ds(0, count)], sem).wait()

    landed[me] = turned[me]
    sums = (jnp.zeros((2 * NARROW, 128), jnp.float32),) * 2
    sums = add(turned[me], sums)
    wait(15, recv_sem.at[0])
    for dz in STEPS[:7]:
        for dc in range(2):
            sums = take(sums, dz, 0, dc)
    sums = take(sums, 0, 0, 1)

    def take_round(round_, sums):
        wait(8, recv_sem.at[1 + round_])
        for step in range(8):
            sums = take(sums, STEPS[step], *over(round_, STEPS[step]))
        return sums

    sums = lax.fori_loop(0, 6, take_round, sums)

    low = jnp.sum(sums[0], axis=1, keepdims=True) * (1.0 / (N * ROWS))
    high = jnp.sum(sums[1], axis=1, keepdims=True) * (1.0 / (N * ROWS))
    stats[0] = jnp.broadcast_to(low, stats.shape[1:])
    stats[1] = jnp.broadcast_to(1.0 / (high - low + 0.1), stats.shape[1:])
    wait(N - 1, send_sem)


def write(landed, stats, first_out, second_out, ready, sem):
    pieces = sem.shape[1]
    each = N // pieces

    def put(which, piece):
        out = (first_out, second_out)[which]
        rows = pl.ds(pl.multiple_of(piece * each * ROWS, each * ROWS), each * ROWS)
        return pltpu.make_async_copy(ready.at[which, :, rows], out.at[:, rows], sem.at[which, piece])

    low, factor = stats[0, :, :1], stats[1, :, :1]

    def finish(piece, carry):
        for i in range(each):
            block = (landed[piece * each + i] - low) * factor
            rows = pl.ds(pl.multiple_of((piece * each + i) * ROWS, ROWS), ROWS)
            ready[0, :, rows] = block[:NARROW]
            ready[1, :, rows] = block[NARROW:]
        put(0, piece).start()
        put(1, piece).start()
        return carry

    lax.fori_loop(0, pieces, finish, 0)

    def drain(piece, carry):
        put(0, piece).wait()
        put(1, piece).wait()
        return carry

    lax.fori_loop(0, pieces, drain, 0)


def shards(samples_in, second_samples_in):
    whole = pltpu.VMEM((N, 2 * NARROW, ROWS), jnp.float32)
    columns = pltpu.VMEM((2, 2 * NARROW, 128), jnp.float32)
    vmem, hbm = pl.BlockSpec(memory_space=pltpu.VMEM), pl.BlockSpec(memory_space=pltpu.HBM)
    landed, stats = pl.pallas_call(
        kernel,
        out_shape=(whole, columns),
        in_specs=[hbm] * 2,
        out_specs=(vmem,) * 2,
        scratch_shapes=[
            pltpu.VMEM((2, ROWS, WIDE), jnp.float32),
            whole,
            pltpu.SemaphoreType.DMA((2, 2, 8)),
            pltpu.SemaphoreType.DMA,
            pltpu.SemaphoreType.DMA((7,)),
            pltpu.SemaphoreType.REGULAR,
            pltpu.SemaphoreType.REGULAR,
            pltpu.SemaphoreType.REGULAR,
            pltpu.SemaphoreType.REGULAR,
        ],
        compiler_params=pltpu.CompilerParams(
            collective_id=0, has_side_effects=True, vmem_limit_bytes=58 * 2**20
        ),
    )(samples_in, second_samples_in)
    out = jax.ShapeDtypeStruct((NARROW, N * ROWS), jnp.float32)
    first, second = pl.pallas_call(
        write,
        out_shape=(out, out),
        in_specs=[vmem] * 2,
        out_specs=(hbm,) * 2,
        scratch_shapes=[
            pltpu.VMEM((2, NARROW, N * ROWS), jnp.float32),
            pltpu.SemaphoreType.DMA((2, 8)),
        ],
        compiler_params=pltpu.CompilerParams(vmem_limit_bytes=16 * 2**20),
    )(landed, stats)
    return first.T, second.T


def solution(mesh):
    placed = (P("batch", "group"), P("batch", "group"))
    return jax.shard_map(
        shards,
        mesh=mesh,
        in_specs=placed,
        out_specs=(P(None, ("group", "batch")), P(None, ("group", "batch"))),
        check_vma=False,
    )
```

```python
import jax
import jax.numpy as jnp
from jax import lax
from jax.experimental import pallas as pl
from jax.experimental.pallas import tpu as pltpu
from jax.sharding import PartitionSpec as P

MESH = pl.DeviceIdType.MESH
N = 64
ROWS, WIDE, NARROW = 256, 2048, 32
STEPS = (1, 7, 2, 6, 3, 5, 4, 0)
PAIR = 4 * NARROW


def kernel(
    a_ref, b_ref, landed, stats, held, turned, in_sem, send_sem, recv_sem, below, above, left, right
):
    me = lax.axis_index("batch")
    z, y, c = me // 8, (me // 2) % 4, me % 2

    def device(dz, dy, dc):
        return ((z + dz) % 8) * 8 + ((y + dy) % 4) * 2 + (c + dc) % 2

    def tell(sem, *offset):
        pl.semaphore_signal(
            sem, inc=1, device_id={"batch": device(*offset)}, device_id_type=MESH
        )

    barrier = pltpu.get_barrier_semaphore()
    neighbours = (
        (1, 0, 0), (1, 0, 1), (7, 0, 0), (7, 0, 1), (0, 0, 1), (0, 1, 0), (0, 3, 0)
    )
    for offset in neighbours:
        tell(barrier, *offset)

    sign = z // 2 % 2 * 2 - 1

    def turned_at(step):
        return (8 + sign * STEPS[step]) % 8

    def first_device(step, other):
        return ((z + turned_at(step)) % 8) * 8 + ((y // 2 + other) % 2) * 4

    def load(which, step, other):
        columns = pl.ds(pl.multiple_of(first_device(step, other) * NARROW, PAIR), PAIR)
        source = (a_ref, b_ref)[which]
        return pltpu.make_async_copy(
            source.at[:, columns], held.at[which, :, columns], in_sem.at[which, other, step]
        )

    for other in range(2):
        for step in range(8):
            for which in range(2):
                load(which, step, other).start()

    def turn(step, other):
        first = first_device(step, other)
        columns = pl.ds(pl.multiple_of(first * NARROW, PAIR), PAIR)
        for which in range(2):
            load(which, step, other).wait()
            block = held[which, :, columns].T
            turned[pl.ds(first, 4), which * NARROW : (which + 1) * NARROW, :] = block.reshape(
                4, NARROW, ROWS
            )

    def send(dz, dy, dc, group):
        to = device(dz, dy, dc)
        pltpu.make_async_remote_copy(
            src_ref=turned.at[to],
            dst_ref=landed.at[me],
            send_sem=send_sem,
            recv_sem=recv_sem.at[group],
            device_id={"batch": to},
            device_id_type=MESH,
        ).start()

    def send_column(step):
        send(turned_at(step), 0, 0, 0)
        send(turned_at(step), 0, 1, 0)

    turn(0, 0)
    pl.semaphore_wait(barrier, len(neighbours))
    tell(below, 1, 0, 0)
    tell(above, 7, 0, 0)
    send_column(0)
    turn(1, 0)
    send_column(1)
    turn(2, 0)
    pl.semaphore_wait(below, 1)
    tell(below, 1, 0, 0)
    pl.semaphore_wait(above, 1)
    tell(above, 7, 0, 0)
    send_column(2)
    turn(3, 0)
    send_column(3)
    turn(4, 0)
    pl.semaphore_wait(below, 1)
    tell(below, 1, 0, 0)
    pl.semaphore_wait(above, 1)
    send_column(4)
    turn(5, 0)
    send_column(5)
    turn(6, 0)
    pl.semaphore_wait(below, 1)
    tell(left, 0, 1, 0)
    tell(right, 0, 3, 0)
    turn(7, 0)
    send_column(6)
    turn(0, 1)
    send(0, 0, 1, 0)
    pl.semaphore_wait(left, 1)
    tell(left, 0, 1, 0)
    pl.semaphore_wait(right, 1)
    for step in range(1, 8):
        turn(step, 1)
    pl.semaphore_wait(left, 1)

    def over(round_, dz):
        m = (dz + 7) % 8
        o = (2 * m + (m // 4) * (13 - 4 * m) + 6 + round_) % 6
        return 1 + o // 2, o % 2

    def send_step(round_, dz):
        dy, dc = over(round_, dz)
        send(dz, dy, dc, 1 + round_)

    def to_half(q, half, k):
        send_step(q, (half * 4 + (z + k) % 4 + 8 - z) % 8)

    for q in range(4):
        for step in range(8):
            send_step(q, turned_at(step))
    for q in (4, 5):
        for half in range(2):
            for k in range(4):
                to_half(q, half, k)

    def add(block, sums):
        low, high = sums
        left, right = block[:, :128], block[:, 128:]
        low = low + (jnp.minimum(left, 1.0) + jnp.minimum(right, 1.0))
        high = high + (jnp.maximum(left, 1.0) + jnp.maximum(right, 1.0))
        return low, high

    def take(sums, dz, dy, dc):
        return add(landed[device(8 - dz, 4 - dy, dc)], sums)

    def wait(count, sem):
        pltpu.make_async_copy(landed.at[pl.ds(0, count)], landed.at[pl.ds(0, count)], sem).wait()

    landed[me] = turned[me]
    sums = (jnp.zeros((2 * NARROW, 128), jnp.float32),) * 2
    sums = add(turned[me], sums)
    wait(15, recv_sem.at[0])
    for dz in STEPS[:7]:
        for dc in range(2):
            sums = take(sums, dz, 0, dc)
    sums = take(sums, 0, 0, 1)

    def take_round(round_, sums):
        wait(8, recv_sem.at[1 + round_])
        for step in range(8):
            sums = take(sums, STEPS[step], *over(round_, STEPS[step]))
        return sums

    sums = lax.fori_loop(0, 6, take_round, sums)

    low = jnp.sum(sums[0], axis=1, keepdims=True) * (1.0 / (N * ROWS))
    high = jnp.sum(sums[1], axis=1, keepdims=True) * (1.0 / (N * ROWS))
    stats[0] = jnp.broadcast_to(low, stats.shape[1:])
    stats[1] = jnp.broadcast_to(1.0 / (high - low + 0.1), stats.shape[1:])
    wait(N - 1, send_sem)


def write(landed, stats, first_out, second_out, ready, sem):
    pieces = sem.shape[1]
    each = N // pieces

    def put(which, piece):
        out = (first_out, second_out)[which]
        rows = pl.ds(pl.multiple_of(piece * each * ROWS, each * ROWS), each * ROWS)
        return pltpu.make_async_copy(ready.at[which, :, rows], out.at[:, rows], sem.at[which, piece])

    low, factor = stats[0], stats[1]

    def finish(piece, carry):
        for i in range(each):
            for side in range(0, ROWS, 128):
                block = (landed[piece * each + i, :, side : side + 128] - low) * factor
                rows = pl.ds(pl.multiple_of((piece * each + i) * ROWS + side, 128), 128)
                ready[0, :, rows] = block[:NARROW]
                ready[1, :, rows] = block[NARROW:]
        put(0, piece).start()
        put(1, piece).start()
        return carry

    lax.fori_loop(0, pieces, finish, 0)

    def drain(piece, carry):
        put(0, piece).wait()
        put(1, piece).wait()
        return carry

    lax.fori_loop(0, pieces, drain, 0)


def shards(samples_in, second_samples_in):
    whole = pltpu.VMEM((N, 2 * NARROW, ROWS), jnp.float32)
    columns = pltpu.VMEM((2, 2 * NARROW, 128), jnp.float32)
    vmem, hbm = pl.BlockSpec(memory_space=pltpu.VMEM), pl.BlockSpec(memory_space=pltpu.HBM)
    landed, stats = pl.pallas_call(
        kernel,
        out_shape=(whole, columns),
        in_specs=[hbm] * 2,
        out_specs=(vmem,) * 2,
        scratch_shapes=[
            pltpu.VMEM((2, ROWS, WIDE), jnp.float32),
            whole,
            pltpu.SemaphoreType.DMA((2, 2, 8)),
            pltpu.SemaphoreType.DMA,
            pltpu.SemaphoreType.DMA((7,)),
            pltpu.SemaphoreType.REGULAR,
            pltpu.SemaphoreType.REGULAR,
            pltpu.SemaphoreType.REGULAR,
            pltpu.SemaphoreType.REGULAR,
        ],
        compiler_params=pltpu.CompilerParams(
            collective_id=0, has_side_effects=True, vmem_limit_bytes=58 * 2**20
        ),
    )(samples_in, second_samples_in)
    out = jax.ShapeDtypeStruct((NARROW, N * ROWS), jnp.float32)
    first, second = pl.pallas_call(
        write,
        out_shape=(out, out),
        in_specs=[vmem] * 2,
        out_specs=(hbm,) * 2,
        scratch_shapes=[
            pltpu.VMEM((2, NARROW, N * ROWS), jnp.float32),
            pltpu.SemaphoreType.DMA((2, 8)),
        ],
        compiler_params=pltpu.CompilerParams(vmem_limit_bytes=16 * 2**20),
    )(landed, stats)
    return first.T, second.T


def solution(mesh):
    placed = (P("batch", "group"), P("batch", "group"))
    return jax.shard_map(
        shards,
        mesh=mesh,
        in_specs=placed,
        out_specs=(P(None, ("group", "batch")), P(None, ("group", "batch"))),
        check_vma=False,
    )
```

```python
import jax
import jax.numpy as jnp
from jax import lax
from jax.experimental import pallas as pl
from jax.experimental.pallas import tpu as pltpu
from jax.sharding import PartitionSpec as P

MESH = pl.DeviceIdType.MESH
N = 64
ROWS, WIDE, NARROW = 256, 2048, 32
STEPS = (1, 7, 2, 6, 3, 5, 4, 0)
PAIR = 4 * NARROW


def kernel(
    a_ref, b_ref, landed, stats, held, turned, in_sem, send_sem, recv_sem, below, above, left, right
):
    me = lax.axis_index("batch")
    z, y, c = me // 8, (me // 2) % 4, me % 2

    def device(dz, dy, dc):
        return ((z + dz) % 8) * 8 + ((y + dy) % 4) * 2 + (c + dc) % 2

    def tell(sem, *offset):
        pl.semaphore_signal(
            sem, inc=1, device_id={"batch": device(*offset)}, device_id_type=MESH
        )

    barrier = pltpu.get_barrier_semaphore()
    neighbours = (
        (1, 0, 0), (1, 0, 1), (7, 0, 0), (7, 0, 1), (0, 0, 1), (0, 1, 0), (0, 3, 0)
    )
    for offset in neighbours:
        tell(barrier, *offset)

    sign = z // 2 % 2 * 2 - 1

    def turned_at(step):
        return (8 + sign * STEPS[step]) % 8

    def first_device(step, other):
        return ((z + turned_at(step)) % 8) * 8 + ((y // 2 + other) % 2) * 4

    def load(which, step, other):
        columns = pl.ds(pl.multiple_of(first_device(step, other) * NARROW, PAIR), PAIR)
        source = (a_ref, b_ref)[which]
        return pltpu.make_async_copy(
            source.at[:, columns], held.at[which, :, columns], in_sem.at[which, other, step]
        )

    for other in range(2):
        for step in range(8):
            for which in range(2):
                load(which, step, other).start()

    def turn(step, other):
        first = first_device(step, other)
        columns = pl.ds(pl.multiple_of(first * NARROW, PAIR), PAIR)
        for which in range(2):
            load(which, step, other).wait()
            block = held[which, :, columns].T
            turned[pl.ds(first, 4), which * NARROW : (which + 1) * NARROW, :] = block.reshape(
                4, NARROW, ROWS
            )

    def send(dz, dy, dc, group):
        to = device(dz, dy, dc)
        pltpu.make_async_remote_copy(
            src_ref=turned.at[to],
            dst_ref=landed.at[me],
            send_sem=send_sem,
            recv_sem=recv_sem.at[group],
            device_id={"batch": to},
            device_id_type=MESH,
        ).start()

    def send_column(step):
        send(turned_at(step), 0, 0, 0)
        send(turned_at(step), 0, 1, 0)

    turn(0, 0)
    pl.semaphore_wait(barrier, len(neighbours))
    tell(below, 1, 0, 0)
    tell(above, 7, 0, 0)
    send_column(0)
    turn(1, 0)
    send_column(1)
    turn(2, 0)
    pl.semaphore_wait(below, 1)
    tell(below, 1, 0, 0)
    pl.semaphore_wait(above, 1)
    tell(above, 7, 0, 0)
    send_column(2)
    turn(3, 0)
    send_column(3)
    turn(4, 0)
    pl.semaphore_wait(below, 1)
    tell(below, 1, 0, 0)
    pl.semaphore_wait(above, 1)
    send_column(4)
    turn(5, 0)
    send_column(5)
    turn(6, 0)
    pl.semaphore_wait(below, 1)
    tell(left, 0, 1, 0)
    tell(right, 0, 3, 0)
    turn(7, 0)
    send_column(6)
    turn(0, 1)
    send(0, 0, 1, 0)
    pl.semaphore_wait(left, 1)
    tell(left, 0, 1, 0)
    pl.semaphore_wait(right, 1)
    for step in range(1, 8):
        turn(step, 1)
    pl.semaphore_wait(left, 1)

    def over(round_, dz):
        m = (dz + 7) % 8
        o = (2 * m + (m // 4) * (13 - 4 * m) + 6 + 5 * round_) % 6
        return 1 + o // 2, o % 2

    def send_step(round_, dz):
        dy, dc = over(round_, dz)
        send(dz, dy, dc, 1 + round_)

    def to_half(q, half, k):
        send_step(q, (half * 4 + (z + k) % 4 + 8 - z) % 8)

    for q in range(4):
        for dz in STEPS:
            send_step(q, dz)
    for q in (4, 5):
        for half in range(2):
            for k in range(4):
                to_half(q, half, k)

    def add(block, sums):
        low, high = sums
        left, right = block[:, :128], block[:, 128:]
        low = low + (jnp.minimum(left, 1.0) + jnp.minimum(right, 1.0))
        high = high + (jnp.maximum(left, 1.0) + jnp.maximum(right, 1.0))
        return low, high

    def take(sums, dz, dy, dc):
        return add(landed[device(8 - dz, 4 - dy, dc)], sums)

    def wait(count, sem):
        pltpu.make_async_copy(landed.at[pl.ds(0, count)], landed.at[pl.ds(0, count)], sem).wait()

    landed[me] = turned[me]
    sums = (jnp.zeros((2 * NARROW, 128), jnp.float32),) * 2
    sums = add(turned[me], sums)
    wait(15, recv_sem.at[0])
    for dz in STEPS[:7]:
        for dc in range(2):
            sums = take(sums, dz, 0, dc)
    sums = take(sums, 0, 0, 1)

    def take_round(round_, sums):
        wait(8, recv_sem.at[1 + round_])
        for step in range(8):
            sums = take(sums, STEPS[step], *over(round_, STEPS[step]))
        return sums

    sums = lax.fori_loop(0, 6, take_round, sums)

    low = jnp.sum(sums[0], axis=1, keepdims=True) * (1.0 / (N * ROWS))
    high = jnp.sum(sums[1], axis=1, keepdims=True) * (1.0 / (N * ROWS))
    stats[0] = jnp.broadcast_to(low, stats.shape[1:])
    stats[1] = jnp.broadcast_to(1.0 / (high - low + 0.1), stats.shape[1:])
    wait(N - 1, send_sem)


def write(landed, stats, first_out, second_out, ready, sem):
    pieces = sem.shape[1]
    each = N // pieces

    def put(which, piece):
        out = (first_out, second_out)[which]
        rows = pl.ds(pl.multiple_of(piece * each * ROWS, each * ROWS), each * ROWS)
        return pltpu.make_async_copy(ready.at[which, :, rows], out.at[:, rows], sem.at[which, piece])

    low, factor = stats[0], stats[1]

    def finish(piece, carry):
        for i in range(each):
            for side in range(0, ROWS, 128):
                block = (landed[piece * each + i, :, side : side + 128] - low) * factor
                rows = pl.ds(pl.multiple_of((piece * each + i) * ROWS + side, 128), 128)
                ready[0, :, rows] = block[:NARROW]
                ready[1, :, rows] = block[NARROW:]
        put(0, piece).start()
        put(1, piece).start()
        return carry

    lax.fori_loop(0, pieces, finish, 0)

    def drain(piece, carry):
        put(0, piece).wait()
        put(1, piece).wait()
        return carry

    lax.fori_loop(0, pieces, drain, 0)


def shards(samples_in, second_samples_in):
    whole = pltpu.VMEM((N, 2 * NARROW, ROWS), jnp.float32)
    columns = pltpu.VMEM((2, 2 * NARROW, 128), jnp.float32)
    vmem, hbm = pl.BlockSpec(memory_space=pltpu.VMEM), pl.BlockSpec(memory_space=pltpu.HBM)
    landed, stats = pl.pallas_call(
        kernel,
        out_shape=(whole, columns),
        in_specs=[hbm] * 2,
        out_specs=(vmem,) * 2,
        scratch_shapes=[
            pltpu.VMEM((2, ROWS, WIDE), jnp.float32),
            whole,
            pltpu.SemaphoreType.DMA((2, 2, 8)),
            pltpu.SemaphoreType.DMA,
            pltpu.SemaphoreType.DMA((7,)),
            pltpu.SemaphoreType.REGULAR,
            pltpu.SemaphoreType.REGULAR,
            pltpu.SemaphoreType.REGULAR,
            pltpu.SemaphoreType.REGULAR,
        ],
        compiler_params=pltpu.CompilerParams(
            collective_id=0, has_side_effects=True, vmem_limit_bytes=58 * 2**20
        ),
    )(samples_in, second_samples_in)
    out = jax.ShapeDtypeStruct((NARROW, N * ROWS), jnp.float32)
    first, second = pl.pallas_call(
        write,
        out_shape=(out, out),
        in_specs=[vmem] * 2,
        out_specs=(hbm,) * 2,
        scratch_shapes=[
            pltpu.VMEM((2, NARROW, N * ROWS), jnp.float32),
            pltpu.SemaphoreType.DMA((2, 8)),
        ],
        compiler_params=pltpu.CompilerParams(vmem_limit_bytes=16 * 2**20),
    )(landed, stats)
    return first.T, second.T


def solution(mesh):
    placed = (P("batch", "group"), P("batch", "group"))
    return jax.shard_map(
        shards,
        mesh=mesh,
        in_specs=placed,
        out_specs=(P(None, ("group", "batch")), P(None, ("group", "batch"))),
        check_vma=False,
    )
```

```python
import jax
import jax.numpy as jnp
from jax import lax
from jax.experimental import pallas as pl
from jax.experimental.pallas import tpu as pltpu
from jax.sharding import PartitionSpec as P

MESH = pl.DeviceIdType.MESH
N = 64
ROWS, WIDE, NARROW = 256, 2048, 32
STEPS = (1, 7, 2, 6, 3, 5, 4, 0)
PAIR = 4 * NARROW


def kernel(
    a_ref, b_ref, landed, stats, held, turned, in_sem, send_sem, recv_sem, below, above, left, right
):
    me = lax.axis_index("batch")
    z, y, c = me // 8, (me // 2) % 4, me % 2

    def device(dz, dy, dc):
        return ((z + dz) % 8) * 8 + ((y + dy) % 4) * 2 + (c + dc) % 2

    def tell(sem, *offset):
        pl.semaphore_signal(
            sem, inc=1, device_id={"batch": device(*offset)}, device_id_type=MESH
        )

    barrier = pltpu.get_barrier_semaphore()
    neighbours = (
        (0, 1, 0), (0, 3, 0), (1, 0, 0), (7, 0, 0), (1, 0, 1), (7, 0, 1), (0, 0, 1)
    )
    for offset in neighbours:
        tell(barrier, *offset)

    sign = z // 2 % 2 * 2 - 1

    def turned_at(step):
        return (8 + sign * STEPS[step]) % 8

    def first_device(step, other):
        return ((z + turned_at(step)) % 8) * 8 + ((y // 2 + other) % 2) * 4

    def load(which, step, other):
        columns = pl.ds(pl.multiple_of(first_device(step, other) * NARROW, PAIR), PAIR)
        source = (a_ref, b_ref)[which]
        return pltpu.make_async_copy(
            source.at[:, columns], held.at[which, :, columns], in_sem.at[which, other, step]
        )

    for other in range(2):
        for step in range(8):
            for which in range(2):
                load(which, step, other).start()

    def turn(step, other):
        first = first_device(step, other)
        columns = pl.ds(pl.multiple_of(first * NARROW, PAIR), PAIR)
        for which in range(2):
            load(which, step, other).wait()
            block = held[which, :, columns].T
            turned[pl.ds(first, 4), which * NARROW : (which + 1) * NARROW, :] = block.reshape(
                4, NARROW, ROWS
            )

    def send(dz, dy, dc, group):
        to = device(dz, dy, dc)
        pltpu.make_async_remote_copy(
            src_ref=turned.at[to],
            dst_ref=landed.at[me],
            send_sem=send_sem,
            recv_sem=recv_sem.at[group],
            device_id={"batch": to},
            device_id_type=MESH,
        ).start()

    def send_column(step):
        send(turned_at(step), 0, 0, 0)
        send(turned_at(step), 0, 1, 0)

    turn(0, 0)
    pl.semaphore_wait(barrier, len(neighbours))
    tell(below, 1, 0, 0)
    tell(above, 7, 0, 0)
    send_column(0)
    turn(1, 0)
    send_column(1)
    turn(2, 0)
    pl.semaphore_wait(below, 1)
    tell(below, 1, 0, 0)
    pl.semaphore_wait(above, 1)
    tell(above, 7, 0, 0)
    send_column(2)
    turn(3, 0)
    send_column(3)
    turn(4, 0)
    pl.semaphore_wait(below, 1)
    tell(below, 1, 0, 0)
    pl.semaphore_wait(above, 1)
    send_column(4)
    turn(5, 0)
    send_column(5)
    turn(6, 0)
    pl.semaphore_wait(below, 1)
    tell(left, 0, 1, 0)
    tell(right, 0, 3, 0)
    turn(7, 0)
    send_column(6)
    turn(0, 1)
    send(0, 0, 1, 0)
    pl.semaphore_wait(left, 1)
    tell(left, 0, 1, 0)
    pl.semaphore_wait(right, 1)
    for step in range(1, 8):
        turn(step, 1)
    pl.semaphore_wait(left, 1)

    def over(round_, dz):
        m = (dz + 7) % 8
        o = (2 * m + (m // 4) * (13 - 4 * m) + 6 + 5 * round_) % 6
        return 1 + o // 2, o % 2

    def send_step(round_, dz):
        dy, dc = over(round_, dz)
        send(dz, dy, dc, 1 + round_)

    def to_half(q, half, k):
        send_step(q, (half * 4 + (z + k) % 4 + 8 - z) % 8)

    for q in range(4):
        for dz in STEPS:
            send_step(q, dz)
    for q in (4, 5):
        for half in range(2):
            for k in range(4):
                to_half(q, half, k)

    def add(block, sums):
        low, high = sums
        left, right = block[:, :128], block[:, 128:]
        low = low + (jnp.minimum(left, 1.0) + jnp.minimum(right, 1.0))
        high = high + (jnp.maximum(left, 1.0) + jnp.maximum(right, 1.0))
        return low, high

    def take(sums, dz, dy, dc):
        return add(landed[device(8 - dz, 4 - dy, dc)], sums)

    def wait(count, sem):
        pltpu.make_async_copy(landed.at[pl.ds(0, count)], landed.at[pl.ds(0, count)], sem).wait()

    landed[me] = turned[me]
    sums = (jnp.zeros((2 * NARROW, 128), jnp.float32),) * 2
    sums = add(turned[me], sums)
    wait(15, recv_sem.at[0])
    for dz in STEPS[:7]:
        for dc in range(2):
            sums = take(sums, dz, 0, dc)
    sums = take(sums, 0, 0, 1)

    def take_round(round_, sums):
        wait(8, recv_sem.at[1 + round_])
        for step in range(8):
            sums = take(sums, STEPS[step], *over(round_, STEPS[step]))
        return sums

    sums = lax.fori_loop(0, 6, take_round, sums)

    low = jnp.sum(sums[0], axis=1, keepdims=True) * (1.0 / (N * ROWS))
    high = jnp.sum(sums[1], axis=1, keepdims=True) * (1.0 / (N * ROWS))
    stats[0] = jnp.broadcast_to(low, stats.shape[1:])
    stats[1] = jnp.broadcast_to(1.0 / (high - low + 0.1), stats.shape[1:])
    wait(N - 1, send_sem)


def write(landed, stats, first_out, second_out, ready, sem):
    pieces = sem.shape[1]
    each = N // pieces

    def put(which, piece):
        out = (first_out, second_out)[which]
        rows = pl.ds(pl.multiple_of(piece * each * ROWS, each * ROWS), each * ROWS)
        return pltpu.make_async_copy(ready.at[which, :, rows], out.at[:, rows], sem.at[which, piece])

    low, factor = stats[0], stats[1]

    def finish(piece, carry):
        for i in range(each):
            for side in range(0, ROWS, 128):
                block = (landed[piece * each + i, :, side : side + 128] - low) * factor
                rows = pl.ds(pl.multiple_of((piece * each + i) * ROWS + side, 128), 128)
                ready[0, :, rows] = block[:NARROW]
                ready[1, :, rows] = block[NARROW:]
        put(0, piece).start()
        put(1, piece).start()
        return carry

    lax.fori_loop(0, pieces, finish, 0)

    def drain(piece, carry):
        put(0, piece).wait()
        put(1, piece).wait()
        return carry

    lax.fori_loop(0, pieces, drain, 0)


def shards(samples_in, second_samples_in):
    whole = pltpu.VMEM((N, 2 * NARROW, ROWS), jnp.float32)
    columns = pltpu.VMEM((2, 2 * NARROW, 128), jnp.float32)
    vmem, hbm = pl.BlockSpec(memory_space=pltpu.VMEM), pl.BlockSpec(memory_space=pltpu.HBM)
    landed, stats = pl.pallas_call(
        kernel,
        out_shape=(whole, columns),
        in_specs=[hbm] * 2,
        out_specs=(vmem,) * 2,
        scratch_shapes=[
            pltpu.VMEM((2, ROWS, WIDE), jnp.float32),
            whole,
            pltpu.SemaphoreType.DMA((2, 2, 8)),
            pltpu.SemaphoreType.DMA,
            pltpu.SemaphoreType.DMA((7,)),
            pltpu.SemaphoreType.REGULAR,
            pltpu.SemaphoreType.REGULAR,
            pltpu.SemaphoreType.REGULAR,
            pltpu.SemaphoreType.REGULAR,
        ],
        compiler_params=pltpu.CompilerParams(
            collective_id=0, has_side_effects=True, vmem_limit_bytes=58 * 2**20
        ),
    )(samples_in, second_samples_in)
    out = jax.ShapeDtypeStruct((NARROW, N * ROWS), jnp.float32)
    first, second = pl.pallas_call(
        write,
        out_shape=(out, out),
        in_specs=[vmem] * 2,
        out_specs=(hbm,) * 2,
        scratch_shapes=[
            pltpu.VMEM((2, NARROW, N * ROWS), jnp.float32),
            pltpu.SemaphoreType.DMA((2, 8)),
        ],
        compiler_params=pltpu.CompilerParams(vmem_limit_bytes=16 * 2**20),
    )(landed, stats)
    return first.T, second.T


def solution(mesh):
    placed = (P("batch", "group"), P("batch", "group"))
    return jax.shard_map(
        shards,
        mesh=mesh,
        in_specs=placed,
        out_specs=(P(None, ("group", "batch")), P(None, ("group", "batch"))),
        check_vma=False,
    )
```
